128 devices in a mesh: dp: 8 (over x_lo, y), expert: 16 (over z, x_hi, core).
Axes of the slice: x: 4 (x_hi: 2, x_lo: 2; x = x_hi * 2 + x_lo), y: 4, z: 4, core: 2. Of those that a mesh axis runs over, the one named last changes fastest.
Arguments:
- tokens: bfloat16 [16384, 1536], P(('dp', 'expert')), may hold values from -6 to 6
- gate_prob: float32 [16384], P(('dp', 'expert')), may hold values from 0.2 to 1
- expert_index: int32 [16384], P(('dp', 'expert')), may hold values from 0 to 31, as said below
- slot_index: int32 [16384], P(('dp', 'expert')), may hold values from 0 to 127, as said below
- dropped: int32 [16384], P(('dp', 'expert')), may hold values from 0 to 1
- cotangent: bfloat16 [16384, 1536], P(('dp', 'expert')), may hold values from -6 to 6
- expert_in: bfloat16 [32, 1536, 6144], P('expert', None, 'dp'), may hold values from -0.15625 to 0.15625
- expert_out: bfloat16 [32, 6144, 1536], P('expert', 'dp'), may hold values from -0.078125 to 0.078125
- residual_in: bfloat16 [1536, 3072], P(None, 'dp'), may hold values from -0.15625 to 0.15625
- residual_out: bfloat16 [3072, 1536], P('dp'), may hold values from -0.109375 to 0.109375
Outputs:
- output: bfloat16 [16384, 1536], P(('dp', 'expert'))
- grad_tokens: bfloat16 [16384, 1536], P(('dp', 'expert'))
- grad_gate: float32 [16384], P(('dp', 'expert'))
- grad_expert_in: bfloat16 [32, 1536, 6144], P('expert', None, 'dp')
- grad_expert_out: bfloat16 [32, 6144, 1536], P('expert', 'dp')
- grad_residual_in: bfloat16 [1536, 3072], P(None, 'dp')
- grad_residual_out: bfloat16 [3072, 1536], P('dp')
The draws below stay inside these ranges and needn't reach their ends.
Inputs may be any that keep to these rules, and one draw needn't show every extreme that they name: `expert_index`: on every device, at least 7 tokens choose one expert, the same expert on all devices, and the tokens in its first 5 slots are not dropped. `slot_index`: on each device the tokens of one expert hold the slots 0 to n - 1 once each, n being their count; dropped tokens take the highest slots of their expert; on some device all tokens choose one expert.
All inputs are finite; a program needn't handle non-finite values.
Results may differ from the reference program's by a relative error of at most 0.018.
Values may be sent and summed in bfloat16 or wider, within the bound.
No kernel may reach another device: no remote copies, remote signals or barrier semaphores. Data moves between devices by JAX's collectives and lax.ppermute only.
A program may use at most 192 MiB of HBM per device.

```python
import jax
import jax.numpy as jnp
from jax import lax

D = 1536
FF_EXP = 6144
FF_RES = 3072
TOK_DEV = 128
EXPERTS = 32
CAP = 5
TOKENS = 16384
N_DP = 8
N_EXPERT = 16


def routing(base_key):
    favored = jax.random.randint(jax.random.fold_in(base_key, 7), (), 0, EXPERTS)
    block_count = TOKENS // TOK_DEV
    crowded = jax.random.randint(jax.random.fold_in(base_key, 13), (), 0, block_count)

    def one_block(block_index):
        block_key = jax.random.fold_in(jax.random.fold_in(base_key, 11), block_index)
        subkeys = jax.random.split(block_key, 4)
        others = jax.random.randint(subkeys[0], (TOK_DEV,), 0, EXPERTS)
        position = jnp.arange(TOK_DEV)
        chosen = jnp.where((position < CAP + 2) | (block_index == crowded), favored, others)
        dropping = (jax.random.randint(subkeys[1], (TOK_DEV,), 0, 8) == 0) & (position >= CAP)
        priority = jax.random.permutation(subkeys[2], TOK_DEV) + jnp.where(dropping, TOK_DEV, 0)
        matching = chosen[:, None] == chosen[None, :]
        slot_rank = jnp.sum(matching & (priority[None, :] < priority[:, None]), axis=1)
        shuffle = jax.random.permutation(subkeys[3], TOK_DEV)
        return (chosen[shuffle].astype(jnp.int32), slot_rank[shuffle].astype(jnp.int32), dropping[shuffle].astype(jnp.int32))
    chosen_all, slots_all, drops_all = jax.vmap(one_block)(jnp.arange(block_count))
    return (chosen_all.reshape(-1), slots_all.reshape(-1), drops_all.reshape(-1))


def draw_expert_index(key, part):
    return routing(key)[0]


def draw_slot_index(key, part):
    return routing(key)[1]


def draw_dropped(key, part):
    return routing(key)[2]


def block_levels(rng, shape, shards, low, high):
    def one(dim, shards_of):
        heights = jax.random.uniform(jax.random.fold_in(jax.random.fold_in(rng, 6), dim), (shards_of,), jnp.float32, low / len(shards), high / len(shards))
        return jnp.repeat(jnp.exp(heights), shape[dim] // shards_of).reshape((-1,) + (1,) * (len(shape) - dim - 1))

    loudness = one(*shards[0])
    for cut in shards[1:]:
        loudness = loudness * one(*cut)
    return loudness


def bell_draw(own_key, dims, deviation, most, shards=(), kind=jnp.bfloat16):
    values = jax.random.normal(own_key, dims, jnp.float32) * deviation
    if len(shards) > 0:
        values = block_levels(own_key, dims, shards, -0.22, 0.18) * values
    return jnp.clip(values, min=-most, max=most).astype(kind)


def setup_inputs(seed: int = 0) -> dict:
    seeds = jax.random.split(jax.random.key(seed), 11)
    tokens = bell_draw(seeds[0], (TOKENS, D), 1.0, 6.0, ((0, 128),))
    gate_prob = jnp.clip(0.2 + 0.8 * jax.random.uniform(seeds[1], (TOKENS,), jnp.float32) ** block_levels(seeds[1], (TOKENS,), ((0, 128),), -0.2, 0.2), 0.2, 1.0)
    expert_index = draw_expert_index(jax.random.fold_in(seeds[10], 71), 0)
    slot_index = draw_slot_index(jax.random.fold_in(seeds[10], 71), 0)
    dropped = draw_dropped(jax.random.fold_in(seeds[10], 71), 0)
    cotangent = bell_draw(seeds[5], (TOKENS, D), 1.0, 6.0, ((0, 128),))
    expert_in = bell_draw(seeds[6], (EXPERTS, D, FF_EXP), D ** -0.5, 0.15625, ((0, 16), (2, 8)))
    expert_out = bell_draw(seeds[7], (EXPERTS, FF_EXP, D), FF_EXP ** -0.5, 0.078125, ((0, 16), (1, 8)))
    residual_in = bell_draw(seeds[8], (D, FF_RES), D ** -0.5, 0.15625, ((1, 8),))
    residual_out = bell_draw(seeds[9], (FF_RES, D), FF_RES ** -0.5, 0.109375, ((0, 8),))
    return {"tokens": tokens, "gate_prob": gate_prob, "expert_index": expert_index, "slot_index": slot_index, "dropped": dropped, "cotangent": cotangent, "expert_in": expert_in, "expert_out": expert_out, "residual_in": residual_in, "residual_out": residual_out}


def gelu_tanh(values):
    return jax.nn.gelu(values, approximate=True)

def sliced_sum(left, right):
    piece_width = left.shape[1] // N_DP
    running = jnp.zeros((left.shape[0], right.shape[1]), jnp.float32)
    for piece_index in range(N_DP):
        start_col = piece_index * piece_width
        partial_term = jnp.dot(left[:, start_col:start_col + piece_width], right[start_col:start_col + piece_width], preferred_element_type=jnp.float32).astype(jnp.bfloat16)
        running = running + lax.optimization_barrier(partial_term).astype(jnp.float32)
    return running

def reference(tokens, gate_prob, expert_index, slot_index, dropped, cotangent, expert_in, expert_out, residual_in, residual_out):
    kept = (dropped == 0) & (slot_index < CAP)
    kept_float = kept.astype(jnp.float32)
    gate_kept = gate_prob * kept_float
    device_rows = N_DP * N_EXPERT * CAP
    source = (jnp.arange(TOKENS) // TOK_DEV).astype(jnp.int32)
    position = jnp.where(kept, expert_index * device_rows + source * CAP + slot_index, EXPERTS * device_rows).astype(jnp.int32)

    def place_rows(values):
        buffer = jnp.zeros((EXPERTS * device_rows + 1, D), jnp.bfloat16)
        return buffer.at[position].set(values)[:-1].reshape(EXPERTS, device_rows, D)

    def fetch_rows(buffer):
        padded = jnp.concatenate([buffer.reshape(-1, D), jnp.zeros((1, D), jnp.bfloat16)], axis=0)
        return padded[position]
    column = place_rows(tokens)
    scaled = (cotangent.astype(jnp.float32) * gate_kept[:, None]).astype(jnp.bfloat16)
    grad_column = place_rows(scaled)

    def per_expert(operands):
        rows_block, grad_block, weight_in, weight_out = operands
        pre_act = jnp.dot(rows_block, weight_in, preferred_element_type=jnp.float32)
        hidden_f, gelu_back = jax.vjp(gelu_tanh, pre_act)
        hidden = hidden_f.astype(jnp.bfloat16)
        result = sliced_sum(hidden, weight_out).astype(jnp.bfloat16)
        grad_hidden = jnp.dot(grad_block, weight_out.T, preferred_element_type=jnp.float32)
        grad_pre = gelu_back(grad_hidden)[0].astype(jnp.bfloat16)
        grad_out = jnp.dot(hidden.T, grad_block, preferred_element_type=jnp.float32).astype(jnp.bfloat16)
        grad_in = jnp.dot(rows_block.T, grad_pre, preferred_element_type=jnp.float32).astype(jnp.bfloat16)
        grad_rows = sliced_sum(grad_pre, weight_in.T).astype(jnp.bfloat16)
        return (result, grad_rows, grad_in, grad_out)
    results, grad_rows, grad_in, grad_out = lax.map(per_expert, (column, grad_column, expert_in, expert_out))
    expert_token = fetch_rows(results).astype(jnp.float32)
    pre_dense = jnp.dot(tokens, residual_in, preferred_element_type=jnp.float32)
    dense_f, dense_back = jax.vjp(gelu_tanh, pre_dense)
    dense_hidden = dense_f.astype(jnp.bfloat16)
    dense_sum = sliced_sum(dense_hidden, residual_out)
    output = (dense_sum + gate_kept[:, None] * expert_token).astype(jnp.bfloat16)
    grad_gate = kept_float * lax.optimization_barrier(jnp.sum(cotangent.astype(jnp.float32) * expert_token, axis=1))
    dense_grad_hidden = jnp.dot(cotangent, residual_out.T, preferred_element_type=jnp.float32)
    dense_grad_pre = dense_back(dense_grad_hidden)[0].astype(jnp.bfloat16)
    grad_res_out = jnp.dot(dense_hidden.T, cotangent, preferred_element_type=jnp.float32).astype(jnp.bfloat16)
    grad_res_in = jnp.dot(tokens.T, dense_grad_pre, preferred_element_type=jnp.float32).astype(jnp.bfloat16)
    dense_dx = sliced_sum(dense_grad_pre, residual_in.T)
    grad_tokens = (dense_dx + fetch_rows(grad_rows).astype(jnp.float32)).astype(jnp.bfloat16)
    return (output, grad_tokens, grad_gate, grad_in, grad_out, grad_res_in, grad_res_out)
```

```python
import jax
import jax.numpy as jnp
from jax import lax
from jax.sharding import Mesh
from jax.sharding import PartitionSpec as P

EXPERT = ("z", "xh", "core")
DP = ("xl", "y")
ALL = DP + EXPERT

SWAP = [(0, 1), (1, 0)]
NEAR = [(0, 1), (1, 0), (2, 3), (3, 2)]
FAR = [(0, 3), (3, 0), (1, 2), (2, 1)]
CUBE = (("y", NEAR), ("y", FAR), ("xl", SWAP))
TURNS = ((0, 1, 2), (1, 2, 0), (2, 0, 1))


def swap(value, link):
    return lax.ppermute(value, link[0], link[1])


def half(value, axis, index):
    return lax.slice_in_dim(value, index, index + 1, axis=axis)


def spread(rows):
    lead, count, width = rows.shape
    third = width // 3
    parts = []
    for k, turn in enumerate(TURNS):
        part = rows[:, None, None, None, :, k * third : (k + 1) * third]
        for f in turn:
            part = jnp.concatenate([part, swap(part, CUBE[f])], axis=1 + f)
        parts.append(part)
    return jnp.concatenate(parts, axis=-1).reshape(lead, 8 * count, width)


def collect(rows):
    lead, count, width = rows.shape
    third = width // 3
    cube = rows.reshape(lead, 2, 2, 2, count // 8, width)
    parts = []
    for k, turn in enumerate(TURNS):
        part = cube[..., k * third : (k + 1) * third]
        for step, f in enumerate(turn):
            came = swap(half(part, 1 + f, 1), CUBE[f])
            part = half(part, 1 + f, 0).astype(jnp.float32) + came.astype(jnp.float32)
            if step < 2:
                part = part.astype(jnp.bfloat16)
        parts.append(part)
    return jnp.concatenate(parts, axis=-1).reshape(lead, count // 8, width)


def reduce_over_expert(partial, first):
    rows, width = partial.shape
    z = lax.axis_index("z")
    bits = {"near": (z & 1) ^ (z >> 1), "far": z >> 1}
    z_links = {"near": ("z", NEAR), "far": ("z", FAR)}
    turn = ("near", "far") if first == "near" else ("far", "near")
    steps = [(lax.axis_index("core"), ("core", SWAP))] + [(bits[n], z_links[n]) for n in turn]
    value = partial.reshape(2, 2, 2, rows // 8, width)
    for axis, (bit, link) in enumerate(steps):
        mine = lax.dynamic_index_in_dim(value, bit, axis).astype(jnp.float32)
        other = lax.dynamic_index_in_dim(value, 1 - bit, axis)
        value = (mine + swap(other, link).astype(jnp.float32)).astype(jnp.bfloat16)
    came = swap(value, ("xh", SWAP)).astype(jnp.float32)
    value = (value.astype(jnp.float32) + came).astype(jnp.bfloat16)
    for axis, (bit, link) in reversed(list(enumerate(steps))):
        came = swap(value, link)
        low = jnp.where(bit == 0, value, came)
        high = jnp.where(bit == 0, came, value)
        value = jnp.concatenate([low, high], axis=axis)
    return value.reshape(rows, width)


def gelu_tanh(values):
    return jax.nn.gelu(values, approximate=True)


def dot(left, right, dims):
    return lax.dot_general(left, right, dims, preferred_element_type=jnp.float32)


ROWS_IN = (((1,), (0,)), ((), ()))
ROWS_OUT = (((1,), (1,)), ((), ()))
OVER_ROWS = (((0,), (0,)), ((), ()))
EACH_IN = (((2,), (1,)), ((0,), (0,)))
EACH_OUT = (((2,), (2,)), ((0,), (0,)))
EACH_OVER = (((1,), (1,)), ((0,), (0,)))


def on_device(
    tokens,
    gate_prob,
    expert_index,
    slot_index,
    dropped,
    cotangent,
    expert_in,
    expert_out,
    residual_in,
    residual_out,
):
    bf16 = jnp.bfloat16
    host_count = lax.axis_size(EXPERT)
    local_count = expert_in.shape[0]
    experts_all = local_count * host_count
    row_count, width = tokens.shape
    capacity = max(2, 5 * row_count // (4 * experts_all))
    own_slots = experts_all * capacity
    kept = (dropped == 0) & (slot_index < capacity)
    kept_float = kept.astype(jnp.float32)
    gate_kept = gate_prob * kept_float
    position = jnp.where(kept, expert_index * capacity + slot_index, -1)
    places = lax.broadcasted_iota(jnp.int32, (own_slots, row_count), 0)
    select = (places == position[None, :]).astype(bf16)
    scaled = (cotangent.astype(jnp.float32) * gate_kept[:, None]).astype(bf16)

    def to_hosts(values):
        return dot(select, values, ROWS_IN).astype(bf16).reshape(host_count, -1, width)

    leaving = jnp.stack([to_hosts(tokens), to_hosts(scaled)], axis=1)
    arrived = lax.all_to_all(leaving, EXPERT, split_axis=0, concat_axis=0, tiled=True)
    arrived = arrived.reshape(host_count, 2, local_count, capacity, width)
    arrived = arrived.transpose(1, 2, 0, 3, 4).reshape(2, local_count, -1, width)

    all_tokens = spread(tokens[None])[0]
    all_cotangent = spread(cotangent[None])[0]
    column = spread(arrived[0])
    grad_column = spread(arrived[1])

    pre_dense = dot(all_tokens, residual_in, ROWS_IN)
    dense_f, dense_back = jax.vjp(gelu_tanh, pre_dense)
    dense_hidden = dense_f.astype(bf16)
    dense_part = dot(dense_hidden, residual_out, ROWS_IN).astype(bf16)
    dense_grad_hidden = dot(all_cotangent, residual_out, ROWS_OUT)
    dense_grad_pre = dense_back(dense_grad_hidden)[0].astype(bf16)
    dense_dx = dot(dense_grad_pre, residual_in, ROWS_OUT).astype(bf16)
    out_partial = dot(dense_hidden, all_cotangent, OVER_ROWS).astype(bf16)
    in_partial = dot(all_tokens, dense_grad_pre, OVER_ROWS).astype(bf16)
    grad_residual_in = reduce_over_expert(in_partial, "near")
    grad_residual_out = reduce_over_expert(out_partial, "far")

    pre_expert = dot(column, expert_in, EACH_IN)
    hidden_f, expert_back = jax.vjp(gelu_tanh, pre_expert)
    hidden = hidden_f.astype(bf16)
    expert_part = dot(hidden, expert_out, EACH_IN).astype(bf16)
    grad_hidden = dot(grad_column, expert_out, EACH_OUT)
    grad_pre = expert_back(grad_hidden)[0].astype(bf16)
    expert_dx = dot(grad_pre, expert_in, EACH_OUT).astype(bf16)
    grad_expert_out = dot(hidden, grad_column, EACH_OVER).astype(bf16)
    grad_expert_in = dot(column, grad_pre, EACH_OVER).astype(bf16)

    def to_tokens(sums):
        sums = sums.astype(bf16).reshape(local_count, host_count, capacity, width)
        back = sums.transpose(1, 0, 2, 3).reshape(host_count, -1, width)
        back = lax.all_to_all(back, EXPERT, split_axis=0, concat_axis=0, tiled=True)
        return dot(select, back.reshape(own_slots, width), OVER_ROWS)

    expert_token = to_tokens(collect(expert_part))
    dense_sum = collect(dense_part[None])[0]
    output = (dense_sum + gate_kept[:, None] * expert_token).astype(bf16)
    grad_gate = kept_float * jnp.sum(cotangent.astype(jnp.float32) * expert_token, axis=1)
    expert_dx_token = to_tokens(collect(expert_dx))
    dense_dx_sum = collect(dense_dx[None])[0]
    grad_tokens = (dense_dx_sum + expert_dx_token).astype(bf16)
    return (
        output,
        grad_tokens,
        grad_gate,
        grad_expert_in,
        grad_expert_out,
        grad_residual_in,
        grad_residual_out,
    )


def solution(mesh):
    finer = Mesh(mesh.devices.reshape(2, 4, 4, 2, 2), ALL)
    in_specs = (
        P(ALL, None),
        P(ALL),
        P(ALL),
        P(ALL),
        P(ALL),
        P(ALL, None),
        P(EXPERT, None, DP),
        P(EXPERT, DP, None),
        P(None, DP),
        P(DP, None),
    )
    out_specs = (
        P(ALL, None),
        P(ALL, None),
        P(ALL),
        P(EXPERT, None, DP),
        P(EXPERT, DP, None),
        P(None, DP),
        P(DP, None),
    )
    return jax.shard_map(
        on_device, mesh=finer, in_specs=in_specs, out_specs=out_specs, check_vma=False
    )
```

```python
import jax
import jax.numpy as jnp
from jax import lax
from jax.experimental import pallas as pl
from jax.experimental.pallas import tpu as pltpu
from jax.sharding import Mesh
from jax.sharding import PartitionSpec as P


EXPERT = ("z", "xh", "core")
DP = ("xl", "y")
ALL = DP + EXPERT

SWAP = [(0, 1), (1, 0)]
NEAR = [(0, 1), (1, 0), (2, 3), (3, 2)]
FAR = [(0, 3), (3, 0), (1, 2), (2, 1)]
CUBE = (("y", NEAR), ("y", FAR), ("xl", SWAP))
TURNS = ((1, 2, 0), (2, 0, 1), (0, 1, 2))


def swap(value, link):
    return lax.ppermute(value, link[0], link[1])


def cuts(count, tile, extra):
    tiles = count // tile
    rows = [tile * (tiles // 3 + ((k - extra) % 3 < tiles % 3)) for k in range(3)]
    assert sum(rows) == count
    return [(sum(rows[:k]), rows[k]) for k in range(3)]


def spread_pieces(arrays, cut):
    each = [cut] * len(arrays)
    parts = []
    for k in range(3):
        own = [a[:, None, at : at + n] for a, (at, n) in zip(arrays, (c[k] for c in each))]
        parts.append(jnp.concatenate(own, axis=2))
    for step in range(3):
        came = []
        for k, turn in enumerate(TURNS):
            came.append(swap(parts[k], CUBE[turn[step]]))
        if step < 2:
            parts = [jnp.concatenate([p, c], axis=1) for p, c in zip(parts, came)]
    return parts, came, each


def spread(arrays, cut):
    lead, _, width = arrays[0].shape
    parts, came, each = spread_pieces(arrays, cut)
    parts = [jnp.concatenate([p, c], axis=1) for p, c in zip(parts, came)]
    whole = []
    for i in range(len(arrays)):
        found = []
        for k in range(3):
            at, n = sum(each[j][k][1] for j in range(i)), each[i][k][1]
            found.append(parts[k][:, :, at : at + n].reshape(lead, 8 * n, width))
        whole.append(jnp.concatenate(found, axis=1))
    return whole


def collect(arrays, cut):
    lead, _, width = arrays[0].shape
    each = [cut] * len(arrays)
    keep, send = [], []
    for k in range(3):
        blocks = []
        for a, c in zip(arrays, each):
            at, n = c[k]
            blocks.append(a[:, 8 * at : 8 * (at + n)].reshape(lead, 8, n, width))
        keep.append([b[:, :4] for b in blocks])
        send.append(jnp.concatenate([b[:, 4:] for b in blocks], axis=2))
    return collect_pieces(keep, send, each)


def collect_pieces(keep, send, each):
    f32, bf16 = jnp.float32, jnp.bfloat16
    for step in range(3):
        came = []
        for k, turn in enumerate(TURNS):
            came.append(swap(send[k], CUBE[turn[2 - step]]))
        if step == 2:
            break
        size = 2 >> step
        for k in range(3):
            low, high, at = [], [], 0
            for b in keep[k]:
                n = b.shape[2]
                c = came[k][:, :, at : at + n]
                own = b[:, size : 2 * size].astype(f32)
                high.append((own + c[:, size:].astype(f32)).astype(bf16))
                low.append((b[:, :size].astype(f32) + c[:, :size].astype(f32)).astype(bf16))
                at += n
            keep[k] = [jnp.concatenate(low, axis=2)]
            send[k] = jnp.concatenate(high, axis=2)
    sums = []
    for i in range(len(each)):
        found = []
        for k in range(3):
            at, n = sum(each[j][k][1] for j in range(i)), each[i][k][1]
            own = keep[k][0][:, 0, at : at + n].astype(f32)
            found.append(own + came[k][:, 0, at : at + n].astype(f32))
        sums.append(jnp.concatenate(found, axis=1))
    return sums


ROOT = 0.7978845608028654
CUBIC = 0.044715


def assemble(pieces, whole):
    at = 0
    for k in range(3):
        for piece in (pieces[k], pieces[3 + k]):
            rows = piece.shape[1] * piece.shape[2]
            whole[0, at : at + rows, :] = piece[0].reshape(rows, piece.shape[3])
            at += rows


def hand_out(total, pieces):
    at = 0
    for k in range(3):
        for piece in (pieces[k], pieces[3 + k]):
            rows = piece.shape[1] * piece.shape[2]
            value = total[at : at + rows, :].astype(jnp.bfloat16)
            piece[0] = value.reshape(piece.shape[1:])
            at += rows


def forward_body(*refs):
    pieces, (w_in, w_out), outs = refs[:6], refs[6:8], refs[8:]
    whole, hidden_out, slope_out = outs[6:]
    assemble(pieces, whole)
    v = dot(whole[0], w_in[0], ROWS_IN)
    square = v * v
    t = jnp.tanh(ROOT * v * (1.0 + CUBIC * square))
    half_one = 0.5 * (1.0 + t)
    hidden = (v * half_one).astype(jnp.bfloat16)
    slope = half_one + 0.5 * v * (1.0 - t * t) * (ROOT * (1.0 + 3.0 * CUBIC * square))
    hidden_out[0] = hidden
    slope_out[0] = slope.astype(jnp.bfloat16)
    hand_out(dot(hidden, w_out[0], ROWS_IN), outs[:6])


def backward_body(*refs):
    pieces, (w_in, w_out, slope), outs = refs[:6], refs[6:9], refs[9:]
    whole, grad_out = outs[6:]
    assemble(pieces, whole)
    grad = dot(whole[0], w_out[0], ROWS_OUT) * slope[0].astype(jnp.float32)
    grad = grad.astype(jnp.bfloat16)
    grad_out[0] = grad
    hand_out(dot(grad, w_in[0], ROWS_OUT), outs[:6])


def expert_call(body, pieces, weights, units_in, units_out, interpret=False):
    lead, width, units = weights[0].shape
    rows = sum(p.shape[1] * p.shape[2] for p in pieces)
    bf16 = jnp.bfloat16
    piece_specs = [pl.BlockSpec((1,) + p.shape[1:], lambda j: (j, 0, 0, 0)) for p in pieces]
    shapes = [(width, units), (units, width)] + [(rows, units)] * len(units_in)
    outs_more = [(rows, width)] + [(rows, units)] * units_out
    outs = pl.pallas_call(
        body,
        grid=(lead,),
        in_specs=piece_specs + [pl.BlockSpec((1,) + s, lambda j: (j, 0, 0)) for s in shapes],
        out_specs=piece_specs + [pl.BlockSpec((1,) + s, lambda j: (j, 0, 0)) for s in outs_more],
        out_shape=[jax.ShapeDtypeStruct(p.shape, bf16) for p in pieces]
        + [jax.ShapeDtypeStruct((lead,) + s, bf16) for s in outs_more],
        compiler_params=pltpu.CompilerParams(
            dimension_semantics=("arbitrary",), vmem_limit_bytes=40 * 2**20
        ),
        cost_estimate=pl.CostEstimate(
            flops=4 * lead * rows * width * units,
            bytes_accessed=8 * lead * (rows * width + units * width),
            transcendentals=0,
        ),
        interpret=interpret,
    )(*pieces, *weights, *units_in)
    return outs[:3], outs[3:6], outs[6:]


def reduce_over_expert(in_partial, out_partial):
    f32, bf16 = jnp.float32, jnp.bfloat16
    rows, width = in_partial.shape
    fold = rows // width
    first = jax.lax.axis_index("core") == 0
    z = lax.axis_index("z")
    folded = out_partial.reshape(width, fold, width).transpose(1, 0, 2)
    inward = in_partial.reshape(fold, width, width)
    came = swap(jnp.where(first, folded, inward), ("core", SWAP))
    mine = jnp.where(first, inward, folded).astype(f32)
    mine = (mine + came.astype(f32)).astype(bf16)
    ways = [[(i, i ^ d) for i in range(4)] for d in (1, 2, 3)]
    quarter = lax.dynamic_index_in_dim(mine, z, 0, keepdims=False).astype(f32)
    leaving = [lax.dynamic_index_in_dim(mine, z ^ d, 0, keepdims=False) for d in (1, 2, 3)]
    came = [swap(v, ("z", way)) for v, way in zip(leaving, ways)]
    quarter = (quarter + sum(c.astype(f32) for c in came)).astype(bf16)
    came = swap(quarter, ("xh", SWAP))
    quarter = (quarter.astype(f32) + came.astype(f32)).astype(bf16)
    all_four = [quarter] + [swap(quarter, ("z", way)) for way in ways]
    odd, upper = (z & 1) == 1, z >= 2
    all_four = [jnp.where(odd, all_four[p ^ 1], all_four[p]) for p in range(4)]
    all_four = [jnp.where(upper, all_four[p ^ 2], all_four[p]) for p in range(4)]
    mine = jnp.stack(all_four)
    came = swap(mine, ("core", SWAP))
    in_total = jnp.where(first, mine, came).reshape(rows, width)
    out_total = jnp.where(first, came, mine).transpose(1, 0, 2).reshape(width, rows)
    return in_total, out_total


def gelu_tanh(values):
    return jax.nn.gelu(values, approximate=True)


def dot(left, right, dims):
    return lax.dot_general(left, right, dims, preferred_element_type=jnp.float32)


ROWS_IN = (((1,), (0,)), ((), ()))
ROWS_OUT = (((1,), (1,)), ((), ()))
OVER_ROWS = (((0,), (0,)), ((), ()))
EACH_OVER = (((1,), (1,)), ((0,), (0,)))


def layer(
    tokens,
    gate_prob,
    expert_index,
    slot_index,
    dropped,
    cotangent,
    expert_in,
    expert_out,
    residual_in,
    residual_out,
):
    bf16 = jnp.bfloat16
    host_count = lax.axis_size(EXPERT)
    local_count = expert_in.shape[0]
    experts_all = local_count * host_count
    row_count, width = tokens.shape
    capacity = max(2, 5 * row_count // (4 * experts_all))
    own_slots = experts_all * capacity
    kept = (dropped == 0) & (slot_index < capacity)
    kept_float = kept.astype(jnp.float32)
    gate_kept = gate_prob * kept_float
    position = jnp.where(kept, expert_index * capacity + slot_index, -1)
    places = lax.broadcasted_iota(jnp.int32, (own_slots, row_count), 0)
    select = (places == position[None, :]).astype(bf16)
    scaled = (cotangent.astype(jnp.float32) * gate_kept[:, None]).astype(bf16)

    def to_hosts(values):
        return dot(select, values, ROWS_IN).astype(bf16).reshape(host_count, -1, width)

    leaving = jnp.stack([to_hosts(tokens), to_hosts(scaled)], axis=1)
    arrived = lax.all_to_all(leaving, EXPERT, split_axis=0, concat_axis=0, tiled=True)
    arrived = arrived.reshape(host_count, 2, local_count, capacity, width)
    arrived = arrived.transpose(1, 2, 0, 3, 4).reshape(2, local_count, -1, width)

    dense_cut = cuts(row_count, 8, 0)
    expert_cut = cuts(host_count * capacity, 16, 0)
    all_tokens, all_cotangent = spread([tokens[None], cotangent[None]], dense_cut)
    all_tokens, all_cotangent = all_tokens[0], all_cotangent[0]
    own_t, came_t, _ = spread_pieces([arrived[0]], expert_cut)
    own_c, came_c, _ = spread_pieces([arrived[1]], expert_cut)

    pre_dense = dot(all_tokens, residual_in, ROWS_IN)
    dense_f, dense_back = jax.vjp(gelu_tanh, pre_dense)
    dense_hidden = dense_f.astype(bf16)
    dense_grad_hidden = dot(all_cotangent, residual_out, ROWS_OUT)
    dense_grad_pre = dense_back(dense_grad_hidden)[0].astype(bf16)
    dense_part = dot(dense_hidden, residual_out, ROWS_IN).astype(bf16)
    dense_dx = dot(dense_grad_pre, residual_in, ROWS_OUT).astype(bf16)
    out_partial = dot(dense_hidden, all_cotangent, OVER_ROWS).astype(bf16)
    in_partial = dot(all_tokens, dense_grad_pre, OVER_ROWS).astype(bf16)
    grad_residual_in, grad_residual_out = reduce_over_expert(in_partial, out_partial)

    keep, send, (column, hidden, slope) = expert_call(
        forward_body, (*own_t, *came_t), (expert_in, expert_out), (), 2
    )
    keep, send = [[v] for v in keep], list(send)
    keep_b, send_b, (grad_column, grad_pre) = expert_call(
        backward_body, (*own_c, *came_c), (expert_in, expert_out), (slope,), 1
    )
    keep_b, send_b = [[v] for v in keep_b], list(send_b)
    grad_expert_out = dot(hidden, grad_column, EACH_OVER).astype(bf16)
    grad_expert_in = dot(column, grad_pre, EACH_OVER).astype(bf16)

    def to_source(sums):
        sums = sums.astype(bf16).reshape(local_count, host_count, capacity, width)
        return sums.transpose(1, 0, 2, 3).reshape(host_count, -1, width)

    dense_sum, dense_dx_sum = collect([dense_part[None], dense_dx[None]], dense_cut)
    (expert_sum,) = collect_pieces(keep, send, [expert_cut])
    (expert_dx_sum,) = collect_pieces(keep_b, send_b, [expert_cut])
    back = jnp.stack([to_source(expert_sum), to_source(expert_dx_sum)], axis=1)
    back = lax.all_to_all(back, EXPERT, split_axis=0, concat_axis=0, tiled=True)
    expert_token = dot(select, back[:, 0].reshape(own_slots, width), OVER_ROWS)
    expert_dx_token = dot(select, back[:, 1].reshape(own_slots, width), OVER_ROWS)
    output = (dense_sum[0] + gate_kept[:, None] * expert_token).astype(bf16)
    grad_gate = kept_float * jnp.sum(cotangent.astype(jnp.float32) * expert_token, axis=1)
    grad_tokens = (dense_dx_sum[0] + expert_dx_token).astype(bf16)
    return (
        output,
        grad_tokens,
        grad_gate,
        grad_expert_in,
        grad_expert_out,
        grad_residual_in,
        grad_residual_out,
    )


def solution(mesh):
    finer = Mesh(mesh.devices.reshape(2, 4, 4, 2, 2), ALL)
    in_specs = (
        P(ALL, None),
        P(ALL),
        P(ALL),
        P(ALL),
        P(ALL),
        P(ALL, None),
        P(EXPERT, None, DP),
        P(EXPERT, DP, None),
        P(None, DP),
        P(DP, None),
    )
    out_specs = (
        P(ALL, None),
        P(ALL, None),
        P(ALL),
        P(EXPERT, None, DP),
        P(EXPERT, DP, None),
        P(None, DP),
        P(DP, None),
    )
    return jax.shard_map(layer, mesh=finer, in_specs=in_specs, out_specs=out_specs, check_vma=False)
```
